256 devices in a mesh: pair: 16 (over y_hi, x, core), tile: 16 (over y_lo, z).
Axes of the slice: x: 4, y: 4 (y_hi: 2, y_lo: 2; y = y_hi * 2 + y_lo), z: 8, core: 2. Of those that a mesh axis runs over, the one named last changes fastest.
Arguments:
- fixed: float32 [32768, 2048], P('pair', 'tile'), parts along dimension 0, may hold values from -6 to 6
- moving: float32 [32768, 2048], P('pair', 'tile'), parts along dimension 0, may hold values from -6 to 6
- offsets: int32 [2, 32768, 2048], P(None, ('pair', 'tile')), parts along dimension 1, may hold values from -3 to 3
- fractions: float32 [2, 32768, 2048], P(None, ('pair', 'tile')), parts along dimension 1, may hold values from 0 to 1
Outputs:
- warped: float32 [32768, 2048], P(('pair', 'tile')), parts along dimension 0
The draws below stay inside these ranges and needn't reach their ends.
There are 16 independent parts, one for each index of `pair`. The reference program is written for one: setup_inputs(seed, part) draws one part's arguments, and reference() takes and returns one part's arrays. A program takes and returns all parts, laid end to end along the dimension named above; each array names one. Nothing has to cross between parts.
All inputs are finite; a program needn't handle non-finite values.
Results may differ from the reference program's by a relative error of at most 0.00002.
Values sent between devices are 32-bit elements; how exact they have to be, the bound alone decides.
A program may use at most 64 MiB of HBM per device.

```python
import jax
import jax.numpy as jnp

RADIUS = 4
REACH = 3
HEIGHT = 2048
WIDTH = 2048


def touch_ends(values, own_key, least, largest):
    place = [jax.random.randint(jax.random.fold_in(own_key, axis), (), 0, length) for axis, length in enumerate(values.shape)]
    longest = values.shape.index(max(values.shape))
    beside = place[:longest] + [(place[longest] + 1) % values.shape[longest]] + place[longest + 1:]
    return values.at[tuple(place)].set(least).at[tuple(beside)].set(largest)


def shard_levels(rng, dims, pieces, least, high):
    gain = 1.0
    for position, shards_of in pieces:
        draws = jax.random.uniform(jax.random.fold_in(jax.random.fold_in(rng, 6), position), (shards_of,), jnp.float32, least / len(pieces), high / len(pieces))
        gain = gain * jnp.repeat(jnp.exp(draws), dims[position] // shards_of).reshape((-1,) + (1,) * (len(dims) - 1 - position))
    return gain


def normal_values(own_key, dims, scale, most, shards=(), kind=jnp.bfloat16):
    values = jax.random.normal(own_key, dims, jnp.float32) * scale
    if len(shards) > 0:
        values = shard_levels(own_key, dims, shards, -0.22, 0.18) * values
    return jnp.clip(values, min=-most, max=most).astype(kind)


def setup_inputs(seed: int = 0, part: int = 0) -> dict:
    keys = jax.random.split(jax.random.key(seed), 5)
    own_keys = jax.random.split(jax.random.fold_in(keys[4], part), 5)
    return {
        "fixed": normal_values(own_keys[0], (HEIGHT, WIDTH), 1.0, 6.0, ((1, 16),), jnp.float32),
        "moving": normal_values(own_keys[1], (HEIGHT, WIDTH), 1.0, 6.0, ((1, 16),), jnp.float32),
        "offsets": touch_ends(jax.random.randint(own_keys[2], (2, HEIGHT, WIDTH), -REACH, REACH + 1), jax.random.fold_in(own_keys[2], 1), -REACH, REACH).astype(jnp.int32),
        "fractions": jnp.clip(1.0 * jax.random.uniform(own_keys[3], (2, HEIGHT, WIDTH), jnp.float32) ** shard_levels(own_keys[3], (2, HEIGHT, WIDTH), ((1, 16),), -0.2, 0.2), 0.0, 1.0),
    }


def window_sum(extended):
    row_total = extended.shape[0] - 2 * RADIUS
    column_total = extended.shape[1] - 2 * RADIUS
    rows_summed = extended[0:row_total, :]
    for shift in range(1, 2 * RADIUS + 1):
        rows_summed = rows_summed + extended[shift:shift + row_total, :]
    result = rows_summed[:, 0:column_total]
    for shift in range(1, 2 * RADIUS + 1):
        result = result + rows_summed[:, shift:shift + column_total]
    return result

def similarity(fixed_ext, moving_ext):
    window_count = float((2 * RADIUS + 1) ** 2)
    fixed_sum = window_sum(fixed_ext)
    moving_sum = window_sum(moving_ext)
    fixed_square = window_sum(fixed_ext * fixed_ext)
    moving_square = window_sum(moving_ext * moving_ext)
    cross_sum = window_sum(fixed_ext * moving_ext)
    fixed_var = fixed_square - fixed_sum * fixed_sum / window_count
    moving_var = moving_square - moving_sum * moving_sum / window_count
    covariance = cross_sum - fixed_sum * moving_sum / window_count
    correlation = covariance / jnp.sqrt(fixed_var * moving_var + 0.001)
    return 0.5 * (1.0 + correlation)

def reference(fixed, moving, offsets, fractions):
    confidence = similarity(jnp.pad(fixed, RADIUS), jnp.pad(moving, RADIUS))
    margin = REACH + 1
    padded = jnp.pad(moving, margin)
    row_index = jnp.arange(HEIGHT, dtype=jnp.int32)[:, None] + offsets[0] + margin
    column_index = jnp.arange(WIDTH, dtype=jnp.int32)[None, :] + offsets[1] + margin
    top_left = padded[row_index, column_index]
    top_right = padded[row_index, column_index + 1]
    bottom_left = padded[row_index + 1, column_index]
    bottom_right = padded[row_index + 1, column_index + 1]
    row_weight = confidence * fractions[0]
    column_weight = confidence * fractions[1]
    upper = (1.0 - column_weight) * top_left + column_weight * top_right
    lower = (1.0 - column_weight) * bottom_left + column_weight * bottom_right
    return (1.0 - row_weight) * upper + row_weight * lower
```

```python
import functools

import jax
import jax.numpy as jnp
from jax import lax
from jax.experimental import pallas as pl
from jax.experimental.pallas import tpu as pltpu
from jax.sharding import PartitionSpec as P

RADIUS = 4
REACH = 3
LANES = 128
GROUP = 8
MESH = pl.DeviceIdType.MESH
COLUMN_SHIFTS = tuple(range(-REACH, REACH + 2))
CHUNKS = (2, 2, 2, 2, 2, 2, 2, 1, 1)


def kernel(
    strips,
    near,
    fixed_ref,
    moving_ref,
    offsets_ref,
    fractions_ref,
    out_ref,
    images,
    shifted,
    sums,
    confidences,
    offsets_buf,
    fractions_buf,
    send_sem,
    recv_sem,
    local_sem,
):
    me = lax.axis_index("tile")
    band = out_ref.shape[0]
    last = strips - 1
    moving_at = strips + 2

    barrier = pltpu.get_barrier_semaphore()
    for step in range(1, strips):
        pl.semaphore_signal(
            barrier, inc=1, device_id={"tile": lax.rem(me + step, strips)}, device_id_type=MESH
        )

    def own_copies(source, target, rows):
        return [
            pltpu.make_async_copy(
                ref.at[pl.ds(source, rows)],
                images.at[base + 1 + me, pl.ds(target, rows)],
                local_sem.at[place],
            )
            for place, (ref, base) in enumerate(((fixed_ref, 0), (moving_ref, moving_at)))
        ]

    whole = band + 2 * RADIUS
    first_own = own_copies(0, RADIUS, whole - RADIUS)
    last_own = own_copies(last * band - RADIUS, 0, whole - RADIUS)
    inner_own = own_copies(jnp.clip(me, 1, last - 1) * band - RADIUS, 0, whole)

    def each_own(act):
        @pl.when(me == 0)
        def _():
            for copy in first_own:
                act(copy)

        @pl.when(me == last)
        def _():
            for copy in last_own:
                act(copy)

        @pl.when(jnp.logical_and(me > 0, me < last))
        def _():
            for copy in inner_own:
                act(copy)

    each_own(lambda copy: copy.start())
    offsets_copy = pltpu.make_async_copy(offsets_ref, offsets_buf, local_sem.at[2])
    fractions_copy = pltpu.make_async_copy(fractions_ref, fractions_buf, local_sem.at[3])
    offsets_copy.start()
    fractions_copy.start()

    for base in (0, moving_at):
        for side in (base, base + strips + 1):
            images[side] = jnp.zeros(images.shape[1:], jnp.float32)

        @pl.when(me == 0)
        def _():
            images[pl.ds(base + 1, strips), 0:RADIUS, :] = jnp.zeros(
                (strips, RADIUS, LANES), jnp.float32
            )

        @pl.when(me == last)
        def _():
            images[pl.ds(base + 1, strips), band + RADIUS : whole, :] = jnp.zeros(
                (strips, RADIUS, LANES), jnp.float32
            )

    for side in (0, strips + 1):
        sums[:, side] = jnp.zeros((sums.shape[0],) + sums.shape[2:], jnp.float32)

    starts = [0]
    for groups in CHUNKS:
        starts.append(max(starts[-1], 2 * RADIUS) + GROUP * groups)
    chunks = len(CHUNKS)

    def target_of(step):
        return lax.rem(me + step, strips)

    def send(chunk, target, skip_top, skip_bottom):
        begin = starts[chunk] + (RADIUS if skip_top else 0)
        rows = starts[chunk + 1] - (RADIUS if skip_bottom else 0) - begin
        for ref, base in ((fixed_ref, 0), (moving_ref, moving_at)):
            pltpu.make_async_remote_copy(
                src_ref=ref.at[pl.ds(target * band - RADIUS + begin, rows)],
                dst_ref=images.at[base + 1 + me, pl.ds(begin, rows)],
                send_sem=send_sem.at[chunk],
                recv_sem=recv_sem.at[chunk],
                device_id={"tile": target},
                device_id_type=MESH,
            ).start()

    def count(sem, blocks, rows):
        piece = images.at[pl.ds(0, blocks), pl.ds(0, rows)]
        pltpu.make_async_copy(piece, piece, sem).wait()

    pl.semaphore_wait(barrier, strips - 1)
    for chunk in range(chunks):
        for target in near(me):
            if chunk == 0:
                pl.when(target == 0)(functools.partial(send, chunk, target, True, False))
                pl.when(target != 0)(functools.partial(send, chunk, target, False, False))
            elif chunk == chunks - 1:
                pl.when(target == last)(functools.partial(send, chunk, target, False, True))
                pl.when(target != last)(functools.partial(send, chunk, target, False, False))
            else:
                send(chunk, target, False, False)

    lane = lax.broadcasted_iota(jnp.int32, (GROUP, LANES), 1)

    def from_right(shift, centre, right):
        return pltpu.roll(jnp.where(lane < shift, right, centre), LANES - shift, 1)

    def from_left(shift, centre, left):
        return pltpu.roll(jnp.where(lane >= LANES - shift, left, centre), shift, 1)

    def make_shifted(row):
        def strip_step(strip, carry):
            left, centre, right = (
                images[moving_at + strip + side, pl.ds(row, GROUP), :] for side in range(3)
            )
            place = 0
            for shift in COLUMN_SHIFTS:
                if shift < 0:
                    value = from_left(-shift, centre, left)
                elif shift > 0:
                    value = from_right(shift, centre, right)
                else:
                    continue
                shifted[place, strip, pl.ds(row, GROUP), :] = value
                place += 1
            return carry

        lax.fori_loop(0, strips, strip_step, 0, unroll=2)

    window_count = float((2 * RADIUS + 1) ** 2)

    def row_sums(row):
        def strip_step(strip, carry):
            totals = [None] * 5
            for step in range(2 * RADIUS + 1):
                f = images[strip + 1, pl.ds(row + step, GROUP), :]
                m = images[moving_at + strip + 1, pl.ds(row + step, GROUP), :]
                for place, term in enumerate((f, m, f * f, m * m, f * m)):
                    totals[place] = term if step == 0 else totals[place] + term
            for place, total in enumerate(totals):
                sums[place, strip + 1] = total
            return carry

        lax.fori_loop(0, strips, strip_step, 0, unroll=2)

    def confidence(row):
        def strip_step(strip, carry):
            windows = []
            for place in range(5):
                left, centre, right = (sums[place, strip + side] for side in range(3))
                total = centre
                for shift in range(1, RADIUS + 1):
                    total = total + (
                        from_left(shift, centre, left) + from_right(shift, centre, right)
                    )
                windows.append(total)
            fixed_sum, moving_sum, fixed_square, moving_square, cross_sum = windows
            fixed_var = fixed_square - fixed_sum * fixed_sum * (1.0 / window_count)
            moving_var = moving_square - moving_sum * moving_sum * (1.0 / window_count)
            covariance = cross_sum - fixed_sum * moving_sum * (1.0 / window_count)
            correlation = covariance * lax.rsqrt(fixed_var * moving_var + 0.001)
            confidences[strip] = 0.5 * (1.0 + correlation)
            return carry

        lax.fori_loop(0, strips, strip_step, 0, unroll=2)

    def pick(values, index):
        for bit in (4, 2, 1):
            chosen = jnp.bitwise_and(index, bit) != 0
            values = [
                jnp.where(chosen, values[place + bit], values[place])
                if place + bit < len(values)
                else values[place]
                for place in range(bit + 1)
            ]
        return values

    def warp(row):
        def strip_step(strip, carry):
            here = (pl.ds(row, GROUP), pl.ds(pl.multiple_of(strip * LANES, LANES), LANES))
            row_index = offsets_buf[(0,) + here] + REACH
            column_index = offsets_buf[(1,) + here] + REACH
            weight = confidences[strip]
            row_weight = weight * fractions_buf[(0,) + here]
            column_weight = weight * fractions_buf[(1,) + here]
            other_weight = 1.0 - column_weight
            blended = []
            for row_shift in COLUMN_SHIFTS:
                rows = pl.ds(row + RADIUS + row_shift, GROUP)
                columns = []
                place = 0
                for shift in COLUMN_SHIFTS:
                    if shift == 0:
                        columns.append(images[moving_at + 1 + strip, rows, :])
                    else:
                        columns.append(shifted[place, strip, rows, :])
                        place += 1
                left, right = pick(columns, column_index)
                blended.append(other_weight * left + column_weight * right)
            upper, lower = pick(blended, row_index)
            out_ref[here] = (1.0 - row_weight) * upper + row_weight * lower
            return carry

        lax.fori_loop(0, strips, strip_step, 0)

    done = 0
    for chunk in range(chunks):
        rows = starts[chunk + 1] - starts[chunk]
        blocks = 2 * (strips - 1)
        if chunk == 0 or chunk == chunks - 1:
            edge = 0 if chunk == 0 else last
            pl.when(me == edge)(
                functools.partial(count, recv_sem.at[chunk], blocks, rows - RADIUS)
            )
            pl.when(me != edge)(functools.partial(count, recv_sem.at[chunk], blocks, rows))
        else:
            count(recv_sem.at[chunk], blocks, rows)
        if chunk == 0:
            each_own(lambda copy: copy.wait())
            offsets_copy.wait()
            fractions_copy.wait()
            make_shifted(0)

        def group_step(group, carry):
            row = pl.multiple_of(group * GROUP, GROUP)
            make_shifted(row + GROUP)
            row_sums(row)
            confidence(row)
            warp(row)
            return carry

        lax.fori_loop(done, done + CHUNKS[chunk], group_step, 0)
        done += CHUNKS[chunk]

    for chunk in range(chunks):
        rows = starts[chunk + 1] - starts[chunk]
        blocks = 2 * (strips - 1)
        if chunk == 0 or chunk == chunks - 1:
            edge = 0 if chunk == 0 else last

            @pl.when(me != edge)
            def _():
                count(send_sem.at[chunk], blocks - 2, rows)
                count(send_sem.at[chunk], 2, rows - RADIUS)

            pl.when(me == edge)(functools.partial(count, send_sem.at[chunk], blocks, rows))
        else:
            count(send_sem.at[chunk], blocks, rows)


def solution(mesh):
    strips = mesh.shape["tile"]
    ring = 8

    def near(me):
        z, y = lax.rem(me, ring), me // ring
        steps = [(0, 1)]
        for far in range(1, ring // 2 + 1):
            for sign in (1, -1) if far < ring // 2 else (1,):
                steps += [(sign * far, 0), (sign * far, 1)]
        return [
            lax.rem(z + dz + ring, ring) + ring * lax.rem(y + dy, strips // ring)
            for dz, dy in steps
        ]

    def on_device(fixed, moving, offsets, fractions):
        band, width = offsets.shape[1:]
        padded = band + 2 * RADIUS + GROUP
        chunks = len(CHUNKS)
        return pl.pallas_call(
            functools.partial(kernel, strips, near),
            out_shape=jax.ShapeDtypeStruct((band, width), jnp.float32),
            in_specs=[pl.BlockSpec(memory_space=pl.ANY)] * 4,
            out_specs=pl.BlockSpec(memory_space=pltpu.VMEM),
            scratch_shapes=[
                pltpu.VMEM((2 * (strips + 2), padded, LANES), jnp.float32),
                pltpu.VMEM((2 * REACH + 1, strips, padded, LANES), jnp.float32),
                pltpu.VMEM((5, strips + 2, GROUP, LANES), jnp.float32),
                pltpu.VMEM((strips, GROUP, LANES), jnp.float32),
                pltpu.VMEM(offsets.shape, offsets.dtype),
                pltpu.VMEM(fractions.shape, fractions.dtype),
                pltpu.SemaphoreType.DMA((chunks,)),
                pltpu.SemaphoreType.DMA((chunks,)),
                pltpu.SemaphoreType.DMA((4,)),
            ],
            compiler_params=pltpu.CompilerParams(
                collective_id=0, has_side_effects=True, vmem_limit_bytes=40 * 2**20
            ),
        )(fixed, moving, offsets, fractions)

    placed = (
        P("pair", "tile"),
        P("pair", "tile"),
        P(None, ("pair", "tile"), None),
        P(None, ("pair", "tile"), None),
    )
    return jax.shard_map(
        on_device, mesh=mesh, in_specs=placed, out_specs=P(("pair", "tile"), None), check_vma=False
    )
```

```python
import functools

import jax
import jax.numpy as jnp
from jax import lax
from jax.experimental import pallas as pl
from jax.experimental.pallas import tpu as pltpu
from jax.sharding import PartitionSpec as P

RADIUS = 4
REACH = 3
LANES = 128
GROUP = 8
MESH = pl.DeviceIdType.MESH
KEPT_SHIFTS = tuple(shift for shift in range(-REACH, REACH + 2) if shift != 0)


def kernel(
    strips,
    near,
    fixed_ref,
    moving_ref,
    offsets_ref,
    fractions_ref,
    out_ref,
    images,
    shifted,
    sums,
    offsets_buf,
    fractions_buf,
    send_sem,
    recv_sem,
    local_sem,
):
    me = lax.axis_index("tile")
    band = out_ref.shape[0]
    last = strips - 1
    moving_at = strips + 2
    whole = band + 2 * RADIUS
    groups = band // GROUP
    chunks = groups // 2 + 1
    pair_rows = 2 * GROUP
    first_rows = pair_rows + 2 * RADIUS

    barrier = pltpu.get_barrier_semaphore()
    for step in range(1, strips):
        pl.semaphore_signal(
            barrier, inc=1, device_id={"tile": lax.rem(me + step, strips)}, device_id_type=MESH
        )
    targets = near(me)

    def send(chunk, begin, rows, target):
        for ref, base in ((fixed_ref, 0), (moving_ref, moving_at)):
            pltpu.make_async_remote_copy(
                src_ref=ref.at[pl.ds(target * band - RADIUS + begin, rows)],
                dst_ref=images.at[base + 1 + me, pl.ds(begin, rows)],
                send_sem=send_sem.at[chunk],
                recv_sem=recv_sem.at[chunk],
                device_id={"tile": target},
                device_id_type=MESH,
            ).start()

    pl.semaphore_wait(barrier, strips - 1)
    for target in targets:
        pl.when(target == 0)(
            functools.partial(send, 0, RADIUS, first_rows - RADIUS, target)
        )
        pl.when(target != 0)(functools.partial(send, 0, 0, first_rows, target))

    def send_pair(chunk, carry):
        for target in targets:
            send(chunk, chunk * pair_rows + 2 * RADIUS, pair_rows, target)
        return carry

    lax.fori_loop(1, chunks - 2, send_pair, 0)
    for target in targets:
        send(chunks - 2, whole - pair_rows, GROUP, target)
    for target in targets:
        pl.when(target == last)(
            functools.partial(send, chunks - 1, whole - GROUP, GROUP - RADIUS, target)
        )
        pl.when(target != last)(
            functools.partial(send, chunks - 1, whole - GROUP, GROUP, target)
        )

    def own_copies(source, target, rows):
        return [
            pltpu.make_async_copy(
                ref.at[pl.ds(source, rows)],
                images.at[base + 1 + me, pl.ds(target, rows)],
                local_sem.at[place],
            )
            for place, (ref, base) in enumerate(((fixed_ref, 0), (moving_ref, moving_at)))
        ]

    first_own = own_copies(0, RADIUS, whole - RADIUS)
    last_own = own_copies(last * band - RADIUS, 0, whole - RADIUS)
    inner_own = own_copies(jnp.clip(me, 1, last - 1) * band - RADIUS, 0, whole)

    def each_own(act):
        @pl.when(me == 0)
        def _():
            for copy in first_own:
                act(copy)

        @pl.when(me == last)
        def _():
            for copy in last_own:
                act(copy)

        @pl.when(jnp.logical_and(me > 0, me < last))
        def _():
            for copy in inner_own:
                act(copy)

    each_own(lambda copy: copy.start())
    offsets_copy = pltpu.make_async_copy(offsets_ref, offsets_buf, local_sem.at[2])
    fractions_copy = pltpu.make_async_copy(fractions_ref, fractions_buf, local_sem.at[3])
    offsets_copy.start()
    fractions_copy.start()

    for base in (0, moving_at):
        for side in (base, base + strips + 1):
            images[side] = jnp.zeros(images.shape[1:], jnp.float32)

        @pl.when(me == 0)
        def _():
            images[pl.ds(base + 1, strips), 0:RADIUS, :] = jnp.zeros(
                (strips, RADIUS, LANES), jnp.float32
            )

        @pl.when(me == last)
        def _():
            images[pl.ds(base + 1, strips), whole - RADIUS : whole, :] = jnp.zeros(
                (strips, RADIUS, LANES), jnp.float32
            )

    each_own(lambda copy: copy.wait())
    offsets_copy.wait()
    fractions_copy.wait()

    lane = lax.broadcasted_iota(jnp.int32, (GROUP, LANES), 1)

    def moved(shift, base, strip, rows):
        centre = images[base + strip + 1, rows, :]
        if shift > 0:
            right = images[base + strip + 2, rows, :]
            return pltpu.roll(jnp.where(lane < shift, right, centre), LANES - shift, 1)
        if shift < 0:
            left = images[base + strip, rows, :]
            return pltpu.roll(jnp.where(lane >= LANES + shift, left, centre), -shift, 1)
        return centre

    def row_sums(row):
        rows = pl.ds(row, GROUP)

        def strip_step(strip, carry):
            totals = [None] * 5
            for shift in range(-RADIUS, RADIUS + 1):
                f = moved(shift, 0, strip, rows)
                m = moved(shift, moving_at, strip, rows)
                if shift in KEPT_SHIFTS:
                    shifted[strip, KEPT_SHIFTS.index(shift), rows, :] = m
                for place, term in enumerate((f, m, f * f, m * m, f * m)):
                    totals[place] = term if shift == -RADIUS else totals[place] + term
            for place, total in enumerate(totals):
                sums[strip, place, rows, :] = total
            return carry

        lax.fori_loop(0, strips, strip_step, 0, unroll=8)

    window_count = float((2 * RADIUS + 1) ** 2)

    def confidence(strip, row):
        windows = []
        for place in range(5):
            total = sums[strip, place, pl.ds(row, GROUP), :]
            for step in range(1, 2 * RADIUS + 1):
                total = total + sums[strip, place, pl.ds(row + step, GROUP), :]
            windows.append(total)
        fixed_sum, moving_sum, fixed_square, moving_square, cross_sum = windows
        fixed_var = fixed_square - fixed_sum * fixed_sum * (1.0 / window_count)
        moving_var = moving_square - moving_sum * moving_sum * (1.0 / window_count)
        covariance = cross_sum - fixed_sum * moving_sum * (1.0 / window_count)
        correlation = covariance * lax.rsqrt(fixed_var * moving_var + 0.001)
        return 0.5 * (1.0 + correlation)

    def pick(values, index):
        for bit in (4, 2, 1):
            chosen = jnp.bitwise_and(index, bit) != 0
            values = [
                jnp.where(chosen, values[place + bit], values[place])
                if place + bit < len(values)
                else values[place]
                for place in range(bit + 1)
            ]
        return values

    def warp(row):
        def strip_step(strip, carry):
            here = (pl.ds(row, GROUP), pl.ds(pl.multiple_of(strip * LANES, LANES), LANES))
            row_index = offsets_buf[(0,) + here] + REACH
            column_index = offsets_buf[(1,) + here] + REACH
            weight = confidence(strip, row)
            row_weight = weight * fractions_buf[(0,) + here]
            column_weight = weight * fractions_buf[(1,) + here]
            other_weight = 1.0 - column_weight
            blended = []
            for row_shift in range(-REACH, REACH + 2):
                rows = pl.ds(row + RADIUS + row_shift, GROUP)
                columns = [
                    shifted[strip, KEPT_SHIFTS.index(shift), rows, :]
                    if shift in KEPT_SHIFTS
                    else images[moving_at + 1 + strip, rows, :]
                    for shift in range(-REACH, REACH + 2)
                ]
                left, right = pick(columns, column_index)
                blended.append(other_weight * left + column_weight * right)
            upper, lower = pick(blended, row_index)
            out_ref[here] = (1.0 - row_weight) * upper + row_weight * lower
            return carry

        lax.fori_loop(0, strips, strip_step, 0)

    def count(sem, blocks, rows):
        piece = images.at[pl.ds(0, blocks), pl.ds(0, rows)]
        pltpu.make_async_copy(piece, piece, sem).wait()

    blocks = 2 * (strips - 1)

    def group_step(group, carry):
        row = pl.multiple_of(group * GROUP, GROUP)

        @pl.when(group == 0)
        def _():
            pl.when(me == 0)(
                functools.partial(count, recv_sem.at[0], blocks, first_rows - RADIUS)
            )
            pl.when(me != 0)(functools.partial(count, recv_sem.at[0], blocks, first_rows))
            row_sums(0)

        @pl.when(
            jnp.logical_and(
                jnp.logical_and(group > 0, group < groups - 2), lax.rem(group, 2) == 0
            )
        )
        def _():
            count(recv_sem.at[group // 2], blocks, pair_rows)

        @pl.when(group == groups - 2)
        def _():
            count(recv_sem.at[chunks - 2], blocks, GROUP)

        @pl.when(group == groups - 1)
        def _():
            pl.when(me == last)(
                functools.partial(count, recv_sem.at[chunks - 1], blocks, GROUP - RADIUS)
            )
            pl.when(me != last)(
                functools.partial(count, recv_sem.at[chunks - 1], blocks, GROUP)
            )

        row_sums(row + GROUP)
        warp(row)
        return carry

    lax.fori_loop(0, groups, group_step, 0)

    def sent(chunk, rows, edge):
        @pl.when(me != edge)
        def _():
            count(send_sem.at[chunk], blocks - 2, rows)
            count(send_sem.at[chunk], 2, rows - RADIUS)

        pl.when(me == edge)(functools.partial(count, send_sem.at[chunk], blocks, rows))

    sent(0, first_rows, 0)
    for chunk in range(1, chunks - 2):
        count(send_sem.at[chunk], blocks, pair_rows)
    count(send_sem.at[chunks - 2], blocks, GROUP)
    sent(chunks - 1, GROUP, last)


def solution(mesh):
    strips = mesh.shape["tile"]
    ring = 8

    def near(me):
        z, y = lax.rem(me, ring), me // ring
        steps = [(0, 1)]
        for far in range(1, ring // 2 + 1):
            for sign in (1, -1) if far < ring // 2 else (1,):
                steps += [(sign * far, 0), (sign * far, 1)]
        return [
            lax.rem(z + dz + ring, ring) + ring * lax.rem(y + dy, strips // ring)
            for dz, dy in steps
        ]

    def on_device(fixed, moving, offsets, fractions):
        band, width = offsets.shape[1:]
        padded = band + 2 * RADIUS + 2 * GROUP
        chunks = band // GROUP // 2 + 1
        return pl.pallas_call(
            functools.partial(kernel, strips, near),
            out_shape=jax.ShapeDtypeStruct((band, width), jnp.float32),
            in_specs=[pl.BlockSpec(memory_space=pl.ANY)] * 4,
            out_specs=pl.BlockSpec(memory_space=pltpu.VMEM),
            scratch_shapes=[
                pltpu.VMEM((2 * (strips + 2), padded, LANES), jnp.float32),
                pltpu.VMEM((strips, len(KEPT_SHIFTS), padded, LANES), jnp.float32),
                pltpu.VMEM((strips, 5, padded, LANES), jnp.float32),
                pltpu.VMEM(offsets.shape, offsets.dtype),
                pltpu.VMEM(fractions.shape, fractions.dtype),
                pltpu.SemaphoreType.DMA((chunks,)),
                pltpu.SemaphoreType.DMA((chunks,)),
                pltpu.SemaphoreType.DMA((4,)),
            ],
            compiler_params=pltpu.CompilerParams(
                collective_id=0, has_side_effects=True, vmem_limit_bytes=63 * 2**20
            ),
        )(fixed, moving, offsets, fractions)

    placed = (
        P("pair", "tile"),
        P("pair", "tile"),
        P(None, ("pair", "tile"), None),
        P(None, ("pair", "tile"), None),
    )
    return jax.shard_map(
        on_device, mesh=mesh, in_specs=placed, out_specs=P(("pair", "tile"), None), check_vma=False
    )
```

```python
import functools

import jax
import jax.numpy as jnp
from jax import lax
from jax.experimental import pallas as pl
from jax.experimental.pallas import tpu as pltpu
from jax.sharding import PartitionSpec as P

RADIUS = 4
REACH = 3
LANES = 128
GROUP = 8
CHUNKS = (4, 4, 4, 2, 1, 1)
MESH = pl.DeviceIdType.MESH
KEPT_SHIFTS = tuple(shift for shift in range(-REACH, REACH + 2) if shift != 0)


def kernel(
    strips,
    fixed_ref,
    moving_ref,
    offsets_ref,
    fractions_ref,
    out_ref,
    images,
    shifted,
    sums,
    offsets_buf,
    fractions_buf,
    send_sem,
    recv_sem,
    local_sem,
    ready_sem,
):
    me = lax.axis_index("tile")
    band = out_ref.shape[0]
    last = strips - 1
    moving_at = strips + 2
    whole = band + 2 * RADIUS
    blocks = 2 * last
    chunks = len(CHUNKS)
    begins = [0] + [2 * RADIUS + GROUP * sum(CHUNKS[: chunk + 1]) for chunk in range(chunks)]

    def send(chunk, target):
        def rows_of(begin, end):
            for ref, base in ((fixed_ref, 0), (moving_ref, moving_at)):
                pltpu.make_async_remote_copy(
                    src_ref=ref.at[pl.ds(target * band - RADIUS + begin, end - begin)],
                    dst_ref=images.at[base + 1 + me, pl.ds(begin, end - begin)],
                    send_sem=send_sem.at[chunk],
                    recv_sem=recv_sem.at[chunk],
                    device_id={"tile": target},
                    device_id_type=MESH,
                ).start()

        begin, end = begins[chunk], begins[chunk + 1]
        if chunk == 0:
            pl.when(target == 0)(lambda: rows_of(begin + RADIUS, end))
            pl.when(target != 0)(lambda: rows_of(begin, end))
        elif chunk == chunks - 1:
            pl.when(target == last)(lambda: rows_of(begin, end - RADIUS))
            pl.when(target != last)(lambda: rows_of(begin, end))
        else:
            rows_of(begin, end)

    ring = strips // 2
    here_z, here_y = lax.rem(me, ring), me // ring

    def target_at(place):
        apart = place + 3
        distance = apart // 4
        way = 1 - 2 * (lax.rem(apart, 4) // 2)
        z = lax.rem(here_z + distance * way + ring, ring)
        return z + ring * lax.rem(here_y + lax.rem(apart, 2), 2)

    def send_range(chunk, low, high, backward=False):
        def step(index, carry):
            send(chunk, target_at(high - 1 - index if backward else low + index))
            return carry

        lax.fori_loop(0, high - low, step, 0)

    barrier = pltpu.get_barrier_semaphore()
    for place in range(5):
        pl.semaphore_signal(
            barrier, inc=1, device_id={"tile": target_at(jnp.int32(place))}, device_id_type=MESH
        )
    pl.semaphore_wait(barrier, 5)

    def tell_beside(phase):
        for place in (1, 3):
            pl.semaphore_signal(
                ready_sem.at[phase],
                inc=1,
                device_id={"tile": target_at(jnp.int32(place))},
                device_id_type=MESH,
            )

    ends = (5, 9, 13, 15)
    tell_beside(0)
    send_range(0, 0, 5)
    send_range(1, 0, 5)
    for phase in range(3):
        pl.semaphore_wait(ready_sem.at[phase], 2)
        if phase < 2:
            tell_beside(phase + 1)
        send_range(0, ends[phase], ends[phase + 1])
    send_range(1, 5, last)
    for chunk in range(2, chunks):
        send_range(chunk, 0, last, backward=chunk == chunks - 1)

    def own_copies(source, target, rows):
        return [
            pltpu.make_async_copy(
                ref.at[pl.ds(source, rows)],
                images.at[base + 1 + me, pl.ds(target, rows)],
                local_sem.at[place],
            )
            for place, (ref, base) in enumerate(((fixed_ref, 0), (moving_ref, moving_at)))
        ]

    first_own = own_copies(0, RADIUS, whole - RADIUS)
    last_own = own_copies(last * band - RADIUS, 0, whole - RADIUS)
    inner_own = own_copies(jnp.clip(me, 1, last - 1) * band - RADIUS, 0, whole)

    def each_own(act):
        @pl.when(me == 0)
        def _():
            for copy in first_own:
                act(copy)

        @pl.when(me == last)
        def _():
            for copy in last_own:
                act(copy)

        @pl.when(jnp.logical_and(me > 0, me < last))
        def _():
            for copy in inner_own:
                act(copy)

    each_own(lambda copy: copy.start())
    offsets_copy = pltpu.make_async_copy(offsets_ref, offsets_buf, local_sem.at[2])
    fractions_copy = pltpu.make_async_copy(fractions_ref, fractions_buf, local_sem.at[3])
    offsets_copy.start()
    fractions_copy.start()

    for base in (0, moving_at):
        for side in (base, base + strips + 1):
            images[side] = jnp.zeros(images.shape[1:], jnp.float32)

        @pl.when(me == 0)
        def _():
            images[pl.ds(base + 1, strips), 0:RADIUS, :] = jnp.zeros(
                (strips, RADIUS, LANES), jnp.float32
            )

        @pl.when(me == last)
        def _():
            images[pl.ds(base + 1, strips), whole - RADIUS : whole, :] = jnp.zeros(
                (strips, RADIUS, LANES), jnp.float32
            )

    each_own(lambda copy: copy.wait())
    offsets_copy.wait()
    fractions_copy.wait()

    lane = lax.broadcasted_iota(jnp.int32, (GROUP, LANES), 1)

    def moved(shift, base, strip, rows):
        centre = images[base + strip + 1, rows, :]
        if shift > 0:
            right = images[base + strip + 2, rows, :]
            return pltpu.roll(jnp.where(lane < shift, right, centre), LANES - shift, 1)
        if shift < 0:
            left = images[base + strip, rows, :]
            return pltpu.roll(jnp.where(lane >= LANES + shift, left, centre), -shift, 1)
        return centre

    def row_sums(row):
        rows = pl.ds(row, GROUP)

        def strip_step(strip, carry):
            totals = [None] * 5
            for shift in range(-RADIUS, RADIUS + 1):
                f = moved(shift, 0, strip, rows)
                m = moved(shift, moving_at, strip, rows)
                if shift in KEPT_SHIFTS:
                    shifted[strip, KEPT_SHIFTS.index(shift), rows, :] = m
                for place, term in enumerate((f, m, f * f, m * m, f * m)):
                    totals[place] = term if shift == -RADIUS else totals[place] + term
            for place, total in enumerate(totals):
                sums[strip, place, rows, :] = total
            return carry

        lax.fori_loop(0, strips, strip_step, 0, unroll=strips)

    window_count = float((2 * RADIUS + 1) ** 2)

    def confidence(strip, row):
        windows = []
        for place in range(5):
            total = sums[strip, place, pl.ds(row, GROUP), :]
            for step in range(1, 2 * RADIUS + 1):
                total = total + sums[strip, place, pl.ds(row + step, GROUP), :]
            windows.append(total)
        fixed_sum, moving_sum, fixed_square, moving_square, cross_sum = windows
        fixed_var = fixed_square - fixed_sum * fixed_sum * (1.0 / window_count)
        moving_var = moving_square - moving_sum * moving_sum * (1.0 / window_count)
        covariance = cross_sum - fixed_sum * moving_sum * (1.0 / window_count)
        correlation = covariance * lax.rsqrt(fixed_var * moving_var + 0.001)
        return 0.5 * (1.0 + correlation)

    def pick(values, index):
        for bit in (4, 2, 1):
            chosen = jnp.bitwise_and(index, bit) != 0
            values = [
                jnp.where(chosen, values[place + bit], values[place])
                if place + bit < len(values)
                else values[place]
                for place in range(bit + 1)
            ]
        return values

    def warp(row):
        def strip_step(strip, carry):
            here = (pl.ds(row, GROUP), pl.ds(pl.multiple_of(strip * LANES, LANES), LANES))
            row_index = offsets_buf[(0,) + here] + REACH
            column_index = offsets_buf[(1,) + here] + REACH
            weight = confidence(strip, row)
            row_weight = weight * fractions_buf[(0,) + here]
            column_weight = weight * fractions_buf[(1,) + here]
            other_weight = 1.0 - column_weight
            blended = []
            for row_shift in range(-REACH, REACH + 2):
                rows = pl.ds(row + RADIUS + row_shift, GROUP)
                columns = [
                    shifted[strip, KEPT_SHIFTS.index(shift), rows, :]
                    if shift in KEPT_SHIFTS
                    else images[moving_at + 1 + strip, rows, :]
                    for shift in range(-REACH, REACH + 2)
                ]
                left, right = pick(columns, column_index)
                blended.append(other_weight * left + column_weight * right)
            upper, lower = pick(blended, row_index)
            out_ref[here] = (1.0 - row_weight) * upper + row_weight * lower
            return carry

        lax.fori_loop(0, strips, strip_step, 0)

    def count(sem, blocks, rows):
        piece = images.at[pl.ds(0, blocks), pl.ds(0, rows)]
        pltpu.make_async_copy(piece, piece, sem).wait()

    def arrived(chunk):
        rows = begins[chunk + 1] - begins[chunk]
        full = functools.partial(count, recv_sem.at[chunk], blocks, rows)
        if chunk in (0, chunks - 1):
            pl.when(me == (last if chunk else 0))(
                functools.partial(count, recv_sem.at[chunk], blocks, rows - RADIUS)
            )
            pl.when(me != (last if chunk else 0))(full)
        else:
            full()

    def sent(chunk):
        rows = begins[chunk + 1] - begins[chunk]
        full = functools.partial(count, send_sem.at[chunk], blocks, rows)
        if chunk in (0, chunks - 1):
            pl.when(me == (last if chunk else 0))(full)

            @pl.when(me != (last if chunk else 0))
            def _():
                count(send_sem.at[chunk], blocks - 2, rows)
                count(send_sem.at[chunk], 2, rows - RADIUS)
        else:
            full()

    def group_step(group, carry):
        row = pl.multiple_of(group * GROUP, GROUP)
        for chunk in range(chunks):

            @pl.when(group == sum(CHUNKS[:chunk]))
            def _():
                arrived(chunk)
                if chunk == 0:
                    row_sums(0)

        row_sums(row + GROUP)
        warp(row)
        return carry

    lax.fori_loop(0, band // GROUP, group_step, 0)
    for chunk in range(chunks):
        sent(chunk)


def solution(mesh):
    strips = mesh.shape["tile"]

    def on_device(fixed, moving, offsets, fractions):
        band, width = offsets.shape[1:]
        padded = band + 2 * RADIUS + 2 * GROUP
        chunks = len(CHUNKS)
        return pl.pallas_call(
            functools.partial(kernel, strips),
            out_shape=pltpu.VMEM((band, width), jnp.float32),
            in_specs=[pl.BlockSpec(memory_space=pltpu.HBM)] * 4,
            out_specs=pl.BlockSpec(memory_space=pltpu.VMEM),
            scratch_shapes=[
                pltpu.VMEM((2 * (strips + 2), padded, LANES), jnp.float32),
                pltpu.VMEM((strips, len(KEPT_SHIFTS), padded, LANES), jnp.float32),
                pltpu.VMEM((strips, 5, padded, LANES), jnp.float32),
                pltpu.VMEM(offsets.shape, offsets.dtype),
                pltpu.VMEM(fractions.shape, fractions.dtype),
                pltpu.SemaphoreType.DMA((chunks,)),
                pltpu.SemaphoreType.DMA((chunks,)),
                pltpu.SemaphoreType.DMA((4,)),
                pltpu.SemaphoreType.REGULAR((3,)),
            ],
            compiler_params=pltpu.CompilerParams(
                collective_id=0, has_side_effects=True, vmem_limit_bytes=60 * 2**20
            ),
        )(fixed, moving, offsets, fractions)

    placed = (
        P("pair", "tile"),
        P("pair", "tile"),
        P(None, ("pair", "tile"), None),
        P(None, ("pair", "tile"), None),
    )
    return jax.shard_map(
        on_device, mesh=mesh, in_specs=placed, out_specs=P(("pair", "tile"), None), check_vma=False
    )
```

```python
import functools

import jax
import jax.numpy as jnp
from jax import lax
from jax.experimental import pallas as pl
from jax.experimental.pallas import tpu as pltpu
from jax.sharding import PartitionSpec as P

RADIUS = 4
REACH = 3
LANES = 128
GROUP = 8
CHUNKS = (4, 4, 4, 2, 1, 1)
MESH = pl.DeviceIdType.MESH
KEPT_SHIFTS = tuple(shift for shift in range(-REACH, REACH + 2) if shift != 0)


def kernel(
    strips,
    fixed_ref,
    moving_ref,
    offsets_ref,
    fractions_ref,
    out_ref,
    images,
    shifted,
    sums,
    triples,
    offsets_buf,
    fractions_buf,
    send_sem,
    recv_sem,
    local_sem,
    ready_sem,
):
    me = lax.axis_index("tile")
    band = out_ref.shape[0]
    last = strips - 1
    moving_at = strips + 2
    whole = band + 2 * RADIUS
    blocks = 2 * last
    chunks = len(CHUNKS)
    begins = [0] + [2 * RADIUS + GROUP * sum(CHUNKS[: chunk + 1]) for chunk in range(chunks)]

    def send(chunk, target):
        def rows_of(begin, end):
            for ref, base in ((fixed_ref, 0), (moving_ref, moving_at)):
                pltpu.make_async_remote_copy(
                    src_ref=ref.at[pl.ds(target * band - RADIUS + begin, end - begin)],
                    dst_ref=images.at[base + 1 + me, pl.ds(begin, end - begin)],
                    send_sem=send_sem.at[chunk],
                    recv_sem=recv_sem.at[chunk],
                    device_id={"tile": target},
                    device_id_type=MESH,
                ).start()

        begin, end = begins[chunk], begins[chunk + 1]
        if chunk == 0:
            pl.when(target == 0)(lambda: rows_of(begin + RADIUS, end))
            pl.when(target != 0)(lambda: rows_of(begin, end))
        elif chunk == chunks - 1:
            pl.when(target == last)(lambda: rows_of(begin, end - RADIUS))
            pl.when(target != last)(lambda: rows_of(begin, end))
        else:
            rows_of(begin, end)

    ring = strips // 2
    here_z, here_y = lax.rem(me, ring), me // ring

    def target_at(place):
        apart = place + 3
        distance = apart // 4
        way = 1 - 2 * (lax.rem(apart, 4) // 2)
        z = lax.rem(here_z + distance * way + ring, ring)
        return z + ring * lax.rem(here_y + lax.rem(apart, 2), 2)

    def send_range(chunk, low, high, backward=False):
        def step(index, carry):
            send(chunk, target_at(high - 1 - index if backward else low + index))
            return carry

        lax.fori_loop(0, high - low, step, 0)

    barrier = pltpu.get_barrier_semaphore()
    for place in range(5):
        pl.semaphore_signal(
            barrier, inc=1, device_id={"tile": target_at(jnp.int32(place))}, device_id_type=MESH
        )
    pl.semaphore_wait(barrier, 5)

    def tell_beside(phase):
        for place in (1, 3):
            pl.semaphore_signal(
                ready_sem.at[phase],
                inc=1,
                device_id={"tile": target_at(jnp.int32(place))},
                device_id_type=MESH,
            )

    ends = (5, 9, 13, 15)
    tell_beside(0)
    send_range(0, 0, 5)
    send_range(1, 0, 5)
    for phase in range(3):
        pl.semaphore_wait(ready_sem.at[phase], 2)
        if phase < 2:
            tell_beside(phase + 1)
        send_range(0, ends[phase], ends[phase + 1])
    send_range(1, 5, last)
    for chunk in range(2, chunks):
        send_range(chunk, 0, last, backward=True)

    def own_copies(source, target, rows):
        return [
            pltpu.make_async_copy(
                ref.at[pl.ds(source, rows)],
                images.at[base + 1 + me, pl.ds(target, rows)],
                local_sem.at[place],
            )
            for place, (ref, base) in enumerate(((fixed_ref, 0), (moving_ref, moving_at)))
        ]

    first_own = own_copies(0, RADIUS, whole - RADIUS)
    last_own = own_copies(last * band - RADIUS, 0, whole - RADIUS)
    inner_own = own_copies(jnp.clip(me, 1, last - 1) * band - RADIUS, 0, whole)

    def each_own(act):
        @pl.when(me == 0)
        def _():
            for copy in first_own:
                act(copy)

        @pl.when(me == last)
        def _():
            for copy in last_own:
                act(copy)

        @pl.when(jnp.logical_and(me > 0, me < last))
        def _():
            for copy in inner_own:
                act(copy)

    each_own(lambda copy: copy.start())
    offsets_copy = pltpu.make_async_copy(offsets_ref, offsets_buf, local_sem.at[2])
    fractions_copy = pltpu.make_async_copy(fractions_ref, fractions_buf, local_sem.at[3])
    offsets_copy.start()
    fractions_copy.start()

    for base in (0, moving_at):
        for side in (base, base + strips + 1):
            images[side] = jnp.zeros(images.shape[1:], jnp.float32)

        @pl.when(me == 0)
        def _():
            images[pl.ds(base + 1, strips), 0:RADIUS, :] = jnp.zeros(
                (strips, RADIUS, LANES), jnp.float32
            )

        @pl.when(me == last)
        def _():
            images[pl.ds(base + 1, strips), whole - RADIUS : whole, :] = jnp.zeros(
                (strips, RADIUS, LANES), jnp.float32
            )

    sums[:, :, 0:GROUP, :] = jnp.zeros((strips, 5, GROUP, LANES), jnp.float32)

    each_own(lambda copy: copy.wait())
    offsets_copy.wait()
    fractions_copy.wait()

    lane = lax.broadcasted_iota(jnp.int32, (GROUP, LANES), 1)

    def moved(shift, base, strip, rows):
        centre = images[base + strip + 1, rows, :]
        if shift > 0:
            right = images[base + strip + 2, rows, :]
            return pltpu.roll(jnp.where(lane < shift, right, centre), LANES - shift, 1)
        if shift < 0:
            left = images[base + strip, rows, :]
            return pltpu.roll(jnp.where(lane >= LANES + shift, left, centre), -shift, 1)
        return centre

    def both_moved(strip, row):
        return [
            [moved(shift, base, strip, pl.ds(row, GROUP)) for base in (0, moving_at)]
            for shift in range(-RADIUS, RADIUS + 1)
        ]

    def row_sums(strip, row, images_moved):
        rows = pl.ds(row, GROUP)
        totals = [None] * 5
        for shift, (f, m) in zip(range(-RADIUS, RADIUS + 1), images_moved):
            if shift in KEPT_SHIFTS:
                shifted[strip, KEPT_SHIFTS.index(shift), rows, :] = m
            for place, term in enumerate((f, m, f * f, m * m, f * m)):
                totals[place] = term if shift == -RADIUS else totals[place] + term
        for place, total in enumerate(totals):
            sums[strip, place, pl.ds(row + GROUP, GROUP), :] = total
            triples[strip, place, pl.ds(row + GROUP - 2, GROUP), :] = total + (
                sums[strip, place, pl.ds(row + GROUP - 1, GROUP), :]
                + sums[strip, place, pl.ds(row + GROUP - 2, GROUP), :]
            )

    window_count = float((2 * RADIUS + 1) ** 2)

    def confidence(strip, row):
        windows = []
        for place in range(5):
            total = triples[strip, place, pl.ds(row + GROUP, GROUP), :]
            for step in (3, 6):
                total = total + triples[strip, place, pl.ds(row + GROUP + step, GROUP), :]
            windows.append(total)
        fixed_sum, moving_sum, fixed_square, moving_square, cross_sum = windows
        fixed_var = fixed_square - fixed_sum * fixed_sum * (1.0 / window_count)
        moving_var = moving_square - moving_sum * moving_sum * (1.0 / window_count)
        covariance = cross_sum - fixed_sum * moving_sum * (1.0 / window_count)
        correlation = covariance * lax.rsqrt(fixed_var * moving_var + 0.001)
        return 0.5 * (1.0 + correlation)

    def pick(values, index):
        for bit in (4, 2, 1):
            chosen = jnp.bitwise_and(index, bit) != 0
            values = [
                jnp.where(chosen, values[place + bit], values[place])
                if place + bit < len(values)
                else values[place]
                for place in range(bit + 1)
            ]
        return values

    def warp(strip, row):
        here = (pl.ds(row, GROUP), pl.ds(pl.multiple_of(strip * LANES, LANES), LANES))
        row_index = offsets_buf[(0,) + here] + REACH
        column_index = offsets_buf[(1,) + here] + REACH
        weight = confidence(strip, row)
        row_weight = weight * fractions_buf[(0,) + here]
        column_weight = weight * fractions_buf[(1,) + here]
        other_weight = 1.0 - column_weight
        blended = []
        for row_shift in range(-REACH, REACH + 2):
            rows = pl.ds(row + RADIUS + row_shift, GROUP)
            columns = [
                shifted[strip, KEPT_SHIFTS.index(shift), rows, :]
                if shift in KEPT_SHIFTS
                else images[moving_at + 1 + strip, rows, :]
                for shift in range(-REACH, REACH + 2)
            ]
            left, right = pick(columns, column_index)
            blended.append(other_weight * left + column_weight * right)
        upper, lower = pick(blended, row_index)
        out_ref[here] = (1.0 - row_weight) * upper + row_weight * lower

    def count(sem, blocks, rows):
        piece = images.at[pl.ds(0, blocks), pl.ds(0, rows)]
        pltpu.make_async_copy(piece, piece, sem).wait()

    def arrived(chunk):
        rows = begins[chunk + 1] - begins[chunk]
        full = functools.partial(count, recv_sem.at[chunk], blocks, rows)
        if chunk in (0, chunks - 1):
            pl.when(me == (last if chunk else 0))(
                functools.partial(count, recv_sem.at[chunk], blocks, rows - RADIUS)
            )
            pl.when(me != (last if chunk else 0))(full)
        else:
            full()

    def sent(chunk):
        rows = begins[chunk + 1] - begins[chunk]
        full = functools.partial(count, send_sem.at[chunk], blocks, rows)
        if chunk in (0, chunks - 1):
            pl.when(me == (last if chunk else 0))(full)

            @pl.when(me != (last if chunk else 0))
            def _():
                count(send_sem.at[chunk], blocks - 2, rows)
                count(send_sem.at[chunk], 2, rows - RADIUS)
        else:
            full()

    def group_step(group, carry):
        row = pl.multiple_of(group * GROUP, GROUP)
        for chunk in range(chunks):

            @pl.when(group == sum(CHUNKS[:chunk]))
            def _():
                arrived(chunk)
                if chunk == 0:

                    def first_step(strip, carry):
                        row_sums(strip, 0, both_moved(strip, 0))
                        return carry

                    lax.fori_loop(0, strips, first_step, 0, unroll=4)

        def sums_step(strip, carry):
            row_sums(strip, row + GROUP, both_moved(strip, row + GROUP))
            return carry

        def warp_step(strip, carry):
            warp(strip, row)
            return carry

        lax.fori_loop(0, strips, sums_step, 0, unroll=16)
        lax.fori_loop(0, strips, warp_step, 0, unroll=4)
        return carry

    lax.fori_loop(0, band // GROUP, group_step, 0)
    for chunk in range(chunks):
        sent(chunk)


def solution(mesh):
    strips = mesh.shape["tile"]

    def on_device(fixed, moving, offsets, fractions):
        band, width = offsets.shape[1:]
        padded = band + 2 * RADIUS + 2 * GROUP
        chunks = len(CHUNKS)
        return pl.pallas_call(
            functools.partial(kernel, strips),
            out_shape=pltpu.VMEM((band, width), jnp.float32),
            in_specs=[pl.BlockSpec(memory_space=pltpu.HBM)] * 4,
            out_specs=pl.BlockSpec(memory_space=pltpu.VMEM),
            scratch_shapes=[
                pltpu.VMEM((2 * (strips + 2), padded, LANES), jnp.float32),
                pltpu.VMEM((strips, len(KEPT_SHIFTS), padded, LANES), jnp.float32),
                pltpu.VMEM((strips, 5, padded, LANES), jnp.float32),
                pltpu.VMEM((strips, 5, padded, LANES), jnp.float32),
                pltpu.VMEM(offsets.shape, offsets.dtype),
                pltpu.VMEM(fractions.shape, fractions.dtype),
                pltpu.SemaphoreType.DMA((chunks,)),
                pltpu.SemaphoreType.DMA((chunks,)),
                pltpu.SemaphoreType.DMA((4,)),
                pltpu.SemaphoreType.REGULAR((3,)),
            ],
            compiler_params=pltpu.CompilerParams(
                collective_id=0, has_side_effects=True, vmem_limit_bytes=60 * 2**20
            ),
        )(fixed, moving, offsets, fractions)

    placed = (
        P("pair", "tile"),
        P("pair", "tile"),
        P(None, ("pair", "tile"), None),
        P(None, ("pair", "tile"), None),
    )
    return jax.shard_map(
        on_device, mesh=mesh, in_specs=placed, out_specs=P(("pair", "tile"), None), check_vma=False
    )
```

```python
import functools

import jax
import jax.numpy as jnp
from jax import lax
from jax.experimental import pallas as pl
from jax.experimental.pallas import tpu as pltpu
from jax.sharding import PartitionSpec as P

RADIUS = 4
REACH = 3
LANES = 128
GROUP = 8
CHUNKS = (4, 4, 4, 1, 1, 1)
MESH = pl.DeviceIdType.MESH
KEPT_SHIFTS = (-3, -2, -1, 1, 2, 3, 4, -4)


def kernel(
    strips,
    fixed_ref,
    moving_ref,
    offsets_ref,
    fractions_ref,
    out_ref,
    images,
    shifted,
    sums,
    triples,
    offsets_buf,
    fractions_buf,
    send_sem,
    recv_sem,
    local_sem,
    ready_sem,
    edge_send_sem,
    edge_recv_sem,
    corner_buf,
):
    me = lax.axis_index("tile")
    band = out_ref.shape[0]
    last = strips - 1
    moving_at = strips + 2
    whole = band + 2 * RADIUS
    blocks = 2 * last
    chunks = len(CHUNKS)
    begins = [RADIUS] + [2 * RADIUS + GROUP * sum(CHUNKS[: chunk + 1]) for chunk in range(chunks)]

    both_images = ((fixed_ref, 0), (moving_ref, moving_at))

    def send(chunk, target, sent_images, place):
        def rows_of(begin, end):
            for ref, base in sent_images:
                pltpu.make_async_remote_copy(
                    src_ref=ref.at[pl.ds(target * band - RADIUS + begin, end - begin)],
                    dst_ref=images.at[base + 1 + me, pl.ds(begin, end - begin)],
                    send_sem=send_sem.at[place],
                    recv_sem=recv_sem.at[place],
                    device_id={"tile": target},
                    device_id_type=MESH,
                ).start()

        rows_of(begins[chunk], begins[chunk + 1])
        if chunk == 0:
            rows_of(begins[-1], whole - RADIUS)

    ring = strips // 2
    here_z, here_y = lax.rem(me, ring), me // ring

    def target_at(place):
        apart = place + 3
        distance = apart // 4
        way = 1 - 2 * (lax.rem(apart, 4) // 2)
        z = lax.rem(here_z + distance * way + ring, ring)
        return z + ring * lax.rem(here_y + lax.rem(apart, 2), 2)

    def send_range(chunk, low, high, backward=False, sent_images=both_images, place=None):
        def step(index, carry):
            target = target_at(high - 1 - index if backward else low + index)
            send(chunk, target, sent_images, chunk if place is None else place)
            return carry

        lax.fori_loop(0, high - low, step, 0)

    barrier = pltpu.get_barrier_semaphore()
    for place in range(5):
        pl.semaphore_signal(
            barrier, inc=1, device_id={"tile": target_at(jnp.int32(place))}, device_id_type=MESH
        )
    pl.semaphore_wait(barrier, 5)

    def tell_beside(phase):
        for place in (1, 3):
            pl.semaphore_signal(
                ready_sem.at[phase],
                inc=1,
                device_id={"tile": target_at(jnp.int32(place))},
                device_id_type=MESH,
            )

    ends = (5, 9, 13, 15)
    tell_beside(0)
    send_range(0, 0, 5)
    send_range(1, 0, 5)
    for phase in range(3):
        pl.semaphore_wait(ready_sem.at[phase], 2)
        if phase < 2:
            tell_beside(phase + 1)
        send_range(0, ends[phase], ends[phase + 1])
    send_range(1, 5, last)

    own_copies = [
        pltpu.make_async_copy(
            ref.at[pl.ds(me * band, band)],
            images.at[base + 1 + me, pl.ds(RADIUS, band)],
            local_sem.at[place],
        )
        for place, (ref, base) in enumerate(((fixed_ref, 0), (moving_ref, moving_at)))
    ]
    for copy in own_copies:
        copy.start()
    offsets_copy = pltpu.make_async_copy(offsets_ref, offsets_buf, local_sem.at[2])
    fractions_copy = pltpu.make_async_copy(fractions_ref, fractions_buf, local_sem.at[3])
    offsets_copy.start()
    fractions_copy.start()

    for base in (0, moving_at):
        for side in (base, base + strips + 1):
            images[side] = jnp.zeros(images.shape[1:], jnp.float32)

        @pl.when(me == 0)
        def _():
            images[pl.ds(base + 1, strips), 0:RADIUS, :] = jnp.zeros(
                (strips, RADIUS, LANES), jnp.float32
            )

        @pl.when(me == last)
        def _():
            images[pl.ds(base + 1, strips), whole - RADIUS : whole, :] = jnp.zeros(
                (strips, RADIUS, LANES), jnp.float32
            )

    sums[:, :, 0:GROUP, :] = jnp.zeros((strips, 5, GROUP, LANES), jnp.float32)

    def count(sem, blocks, rows):
        piece = images.at[pl.ds(0, blocks), pl.ds(0, rows)]
        pltpu.make_async_copy(piece, piece, sem).wait()

    def chunk_rows(chunk):
        return begins[chunk + 1] - begins[chunk] + (RADIUS if chunk == 0 else 0)

    def passed_on(beside, source, target, place):
        return [
            pltpu.make_async_remote_copy(
                src_ref=images.at[pl.ds(base + 1, strips), pl.ds(source, RADIUS)],
                dst_ref=images.at[pl.ds(base + 1, strips), pl.ds(target, RADIUS)],
                send_sem=edge_send_sem.at[place],
                recv_sem=edge_recv_sem.at[place],
                device_id={"tile": beside},
                device_id_type=MESH,
            )
            for base in (0, moving_at)
        ]

    for copy in own_copies:
        copy.wait()
    count(recv_sem.at[0], blocks, chunk_rows(0))

    @pl.when(me > 0)
    def _():
        for copy in passed_on(me - 1, RADIUS, whole - RADIUS, 0):
            copy.start()

    @pl.when(me < last)
    def _():
        for copy in passed_on(me + 1, whole - 2 * RADIUS, 0, 1):
            copy.start()

    for chunk in range(2, chunks - 1):
        send_range(chunk, 0, last, backward=True)
    send_range(chunks - 1, 0, last, True, both_images[1:], chunks - 1)
    send_range(chunks - 1, 0, last, True, both_images[:1], chunks)
    offsets_copy.wait()
    fractions_copy.wait()

    lane = lax.broadcasted_iota(jnp.int32, (GROUP, LANES), 1)

    def moved(shift, base, strip, rows):
        centre = images[base + strip + 1, rows, :]
        if shift > 0:
            right = images[base + strip + 2, rows, :]
            return pltpu.roll(jnp.where(lane < shift, right, centre), LANES - shift, 1)
        if shift < 0:
            left = images[base + strip, rows, :]
            return pltpu.roll(jnp.where(lane >= LANES + shift, left, centre), -shift, 1)
        return centre

    shifts = range(-RADIUS, RADIUS + 1)

    def image_moved(base, strip, row):
        return [moved(shift, base, strip, pl.ds(row, GROUP)) for shift in shifts]

    def moved_before(strip, row):
        rows = pl.ds(row, GROUP)
        return [
            shifted[strip, KEPT_SHIFTS.index(shift), rows, :]
            if shift
            else images[moving_at + 1 + strip, rows, :]
            for shift in shifts
        ]

    def keep(strip, row, moving_moved, kept):
        for shift, m in zip(shifts, moving_moved):
            if shift in kept:
                shifted[strip, KEPT_SHIFTS.index(shift), pl.ds(row, GROUP), :] = m

    def sums_of_three(strip, row):
        for place in range(5):
            triples[strip, place, pl.ds(row + GROUP - 2, GROUP), :] = (
                sums[strip, place, pl.ds(row + GROUP, GROUP), :]
                + sums[strip, place, pl.ds(row + GROUP - 1, GROUP), :]
                + sums[strip, place, pl.ds(row + GROUP - 2, GROUP), :]
            )

    def store_sums(strip, row, terms_of_shifts):
        totals = {}
        for terms in terms_of_shifts:
            for place, term in terms.items():
                totals[place] = totals[place] + term if place in totals else term
        for place, total in totals.items():
            sums[strip, place, pl.ds(row + GROUP, GROUP), :] = total

    def row_sums(strip, row):
        fixed_moved = image_moved(0, strip, row)
        moving_moved = image_moved(moving_at, strip, row)
        keep(strip, row, moving_moved, KEPT_SHIFTS[:-1])
        store_sums(
            strip,
            row,
            [
                {0: f, 1: m, 2: f * f, 3: m * m, 4: f * m}
                for f, m in zip(fixed_moved, moving_moved)
            ],
        )

    def row_sums_of_moving(strip, row):
        moving_moved = image_moved(moving_at, strip, row)
        keep(strip, row, moving_moved, KEPT_SHIFTS)
        store_sums(strip, row, [{1: m, 3: m * m} for m in moving_moved])

    def row_sums_with_fixed(strip, row):
        pairs = zip(image_moved(0, strip, row), moved_before(strip, row))
        store_sums(strip, row, [{0: f, 2: f * f, 4: f * m} for f, m in pairs])

    window_count = float((2 * RADIUS + 1) ** 2)

    def confidence(strip, row):
        windows = []
        for place in range(5):
            total = triples[strip, place, pl.ds(row + GROUP, GROUP), :]
            for step in (3, 6):
                total = total + triples[strip, place, pl.ds(row + GROUP + step, GROUP), :]
            windows.append(total)
        fixed_sum, moving_sum, fixed_square, moving_square, cross_sum = windows
        fixed_var = fixed_square - fixed_sum * fixed_sum * (1.0 / window_count)
        moving_var = moving_square - moving_sum * moving_sum * (1.0 / window_count)
        covariance = cross_sum - fixed_sum * moving_sum * (1.0 / window_count)
        correlation = covariance * lax.rsqrt(fixed_var * moving_var + 0.001)
        return 0.5 * (1.0 + correlation)

    def pick(values, index):
        for bit in (4, 2, 1):
            chosen = jnp.bitwise_and(index, bit) != 0
            values = [
                jnp.where(chosen, values[place + bit], values[place])
                if place + bit < len(values)
                else values[place]
                for place in range(bit + 1)
            ]
        return values

    def band_place(strip, row):
        return pl.ds(row, GROUP), pl.ds(pl.multiple_of(strip * LANES, LANES), LANES)

    def corners(strip, row):
        here = band_place(strip, row)
        column_index = offsets_buf[(1,) + here] + REACH
        row_index = offsets_buf[(0,) + here] + REACH
        lefts, rights = [], []
        for row_shift in range(-REACH, REACH + 2):
            columns = moved_before(strip, row + RADIUS + row_shift)
            left, right = pick(columns[RADIUS - REACH :], column_index)
            lefts.append(left)
            rights.append(right)
        return pick(lefts, row_index) + pick(rights, row_index)

    def blend(strip, row, top_left, bottom_left, top_right, bottom_right):
        here = band_place(strip, row)
        weight = confidence(strip, row)
        row_weight = weight * fractions_buf[(0,) + here]
        column_weight = weight * fractions_buf[(1,) + here]
        upper = (1.0 - column_weight) * top_left + column_weight * top_right
        lower = (1.0 - column_weight) * bottom_left + column_weight * bottom_right
        out_ref[here] = (1.0 - row_weight) * upper + row_weight * lower

    def group_step(group, carry):
        row = pl.multiple_of(group * GROUP, GROUP)
        for chunk in range(1, chunks - 1):
            pl.when(group == sum(CHUNKS[:chunk]))(
                functools.partial(count, recv_sem.at[chunk], blocks, chunk_rows(chunk))
            )

        def sums_step(strip, carry):
            row_sums(strip, row + GROUP)
            sums_of_three(strip, row + GROUP)
            return carry

        def warp_step(strip, carry):
            blend(strip, row, *corners(strip, row))
            return carry

        lax.fori_loop(0, strips, sums_step, 0, unroll=16)
        lax.fori_loop(0, strips, warp_step, 0, unroll=4)
        return carry

    pl.when(me < last)(functools.partial(count, edge_recv_sem.at[0], 2 * strips, RADIUS))
    pl.when(me > 0)(functools.partial(count, edge_recv_sem.at[1], 2 * strips, RADIUS))

    def edge_step(strip, carry):
        row_sums(strip, 0)
        sums_of_three(strip, 0)
        row_sums(strip, band)
        return carry

    lax.fori_loop(0, strips, edge_step, 0, unroll=2)
    lax.fori_loop(0, band // GROUP - 2, group_step, 0)

    last_rows = band - GROUP
    last_groups = (band - 2 * GROUP, band - GROUP)

    def moving_step(strip, carry):
        row_sums_of_moving(strip, last_rows)
        return carry

    def corner_step(strip, carry):
        for group, row in enumerate(last_groups):
            for place, value in enumerate(corners(strip, row)):
                corner_buf[group, place, strip] = value
        return carry

    def fixed_step(strip, carry):
        row_sums_with_fixed(strip, last_rows)
        sums_of_three(strip, last_rows)
        sums_of_three(strip, band)
        return carry

    def blend_step(strip, carry):
        for group, row in enumerate(last_groups):
            blend(strip, row, *(corner_buf[group, place, strip] for place in range(4)))
        return carry

    count(recv_sem.at[chunks - 1], blocks // 2, chunk_rows(chunks - 1))
    lax.fori_loop(0, strips, moving_step, 0, unroll=8)
    lax.fori_loop(0, strips, corner_step, 0, unroll=2)
    count(recv_sem.at[chunks], blocks // 2, chunk_rows(chunks - 1))
    lax.fori_loop(0, strips, fixed_step, 0, unroll=16)
    lax.fori_loop(0, strips, blend_step, 0, unroll=4)

    pl.when(me > 0)(functools.partial(count, edge_send_sem.at[0], 2 * strips, RADIUS))
    pl.when(me < last)(functools.partial(count, edge_send_sem.at[1], 2 * strips, RADIUS))
    for chunk in range(chunks - 1):
        count(send_sem.at[chunk], blocks, chunk_rows(chunk))
    for place in (chunks - 1, chunks):
        count(send_sem.at[place], blocks // 2, chunk_rows(chunks - 1))


def solution(mesh):
    strips = mesh.shape["tile"]

    def on_device(fixed, moving, offsets, fractions):
        band, width = offsets.shape[1:]
        padded = band + 2 * RADIUS + 2 * GROUP
        chunks = len(CHUNKS)
        return pl.pallas_call(
            functools.partial(kernel, strips),
            out_shape=pltpu.VMEM((band, width), jnp.float32),
            in_specs=[pl.BlockSpec(memory_space=pltpu.HBM)] * 4,
            out_specs=pl.BlockSpec(memory_space=pltpu.VMEM),
            scratch_shapes=[
                pltpu.VMEM((2 * (strips + 2), padded, LANES), jnp.float32),
                pltpu.VMEM((strips, len(KEPT_SHIFTS), padded, LANES), jnp.float32),
                pltpu.VMEM((strips, 5, padded, LANES), jnp.float32),
                pltpu.VMEM((strips, 5, padded, LANES), jnp.float32),
                pltpu.VMEM(offsets.shape, offsets.dtype),
                pltpu.VMEM(fractions.shape, fractions.dtype),
                pltpu.SemaphoreType.DMA((chunks + 1,)),
                pltpu.SemaphoreType.DMA((chunks + 1,)),
                pltpu.SemaphoreType.DMA((4,)),
                pltpu.SemaphoreType.REGULAR((3,)),
                pltpu.SemaphoreType.DMA((2,)),
                pltpu.SemaphoreType.DMA((2,)),
                pltpu.VMEM((2, 4, strips, GROUP, LANES), jnp.float32),
            ],
            compiler_params=pltpu.CompilerParams(
                collective_id=0, has_side_effects=True, vmem_limit_bytes=60 * 2**20
            ),
        )(fixed, moving, offsets, fractions)

    placed = (
        P("pair", "tile"),
        P("pair", "tile"),
        P(None, ("pair", "tile"), None),
        P(None, ("pair", "tile"), None),
    )
    return jax.shard_map(
        on_device, mesh=mesh, in_specs=placed, out_specs=P(("pair", "tile"), None), check_vma=False
    )
```

```python
import functools

import jax
import jax.numpy as jnp
from jax import lax
from jax.experimental import pallas as pl
from jax.experimental.pallas import tpu as pltpu
from jax.sharding import PartitionSpec as P

RADIUS = 4
REACH = 3
LANES = 128
GROUP = 8
CHUNKS = (4, 4, 4, 1, 1, 1)
MESH = pl.DeviceIdType.MESH
KEPT_SHIFTS = (-3, -2, -1, 1, 2, 3, 4, -4)


def kernel(
    strips,
    fixed_ref,
    moving_ref,
    offsets_ref,
    fractions_ref,
    out_ref,
    images,
    shifted,
    sums,
    triples,
    offsets_buf,
    fractions_buf,
    send_sem,
    recv_sem,
    local_sem,
    ready_sem,
    edge_send_sem,
    edge_recv_sem,
    corner_buf,
):
    me = lax.axis_index("tile")
    band = out_ref.shape[0]
    last = strips - 1
    moving_at = strips + 2
    whole = band + 2 * RADIUS
    blocks = 2 * last
    chunks = len(CHUNKS)
    begins = [RADIUS] + [2 * RADIUS + GROUP * sum(CHUNKS[: chunk + 1]) for chunk in range(chunks)]

    both_images = ((fixed_ref, 0), (moving_ref, moving_at))

    def send(chunk, target, sent_images, place):
        def rows_of(begin, end):
            for ref, base in sent_images:
                pltpu.make_async_remote_copy(
                    src_ref=ref.at[pl.ds(target * band - RADIUS + begin, end - begin)],
                    dst_ref=images.at[base + 1 + me, pl.ds(begin, end - begin)],
                    send_sem=send_sem.at[place],
                    recv_sem=recv_sem.at[place],
                    device_id={"tile": target},
                    device_id_type=MESH,
                ).start()

        rows_of(begins[chunk], begins[chunk + 1])
        if chunk == 0:
            rows_of(begins[-1], whole - RADIUS)

    ring = strips // 2
    here_z, here_y = lax.rem(me, ring), me // ring

    def target_at(place):
        apart = place + 3
        distance = apart // 4
        way = 1 - 2 * (lax.rem(apart, 4) // 2)
        z = lax.rem(here_z + distance * way + ring, ring)
        return z + ring * lax.rem(here_y + lax.rem(apart, 2), 2)

    def send_range(chunk, low, high, backward=False, sent_images=both_images, place=None):
        def step(index, carry):
            target = target_at(high - 1 - index if backward else low + index)
            send(chunk, target, sent_images, chunk if place is None else place)
            return carry

        lax.fori_loop(0, high - low, step, 0)

    barrier = pltpu.get_barrier_semaphore()
    for place in range(5):
        pl.semaphore_signal(
            barrier, inc=1, device_id={"tile": target_at(jnp.int32(place))}, device_id_type=MESH
        )
    pl.semaphore_wait(barrier, 5)

    def tell_beside(phase):
        for place in (1, 3):
            pl.semaphore_signal(
                ready_sem.at[phase],
                inc=1,
                device_id={"tile": target_at(jnp.int32(place))},
                device_id_type=MESH,
            )

    ends = (5, 9, 13, 15)
    tell_beside(0)
    send_range(0, 0, 5)
    send_range(1, 0, 5)
    for phase in range(3):
        pl.semaphore_wait(ready_sem.at[phase], 2)
        if phase < 2:
            tell_beside(phase + 1)
        send_range(0, ends[phase], ends[phase + 1])
    send_range(1, 5, last)

    own_copies = [
        pltpu.make_async_copy(
            ref.at[pl.ds(me * band, band)],
            images.at[base + 1 + me, pl.ds(RADIUS, band)],
            local_sem.at[place],
        )
        for place, (ref, base) in enumerate(((fixed_ref, 0), (moving_ref, moving_at)))
    ]
    for copy in own_copies:
        copy.start()
    offsets_copy = pltpu.make_async_copy(offsets_ref, offsets_buf, local_sem.at[2])
    fractions_copy = pltpu.make_async_copy(fractions_ref, fractions_buf, local_sem.at[3])
    offsets_copy.start()
    fractions_copy.start()

    for base in (0, moving_at):
        for side in (base, base + strips + 1):
            images[side] = jnp.zeros(images.shape[1:], jnp.float32)

        @pl.when(me == 0)
        def _():
            images[pl.ds(base + 1, strips), 0:RADIUS, :] = jnp.zeros(
                (strips, RADIUS, LANES), jnp.float32
            )

        @pl.when(me == last)
        def _():
            images[pl.ds(base + 1, strips), whole - RADIUS : whole, :] = jnp.zeros(
                (strips, RADIUS, LANES), jnp.float32
            )

    sums[:, :, 0:GROUP, :] = jnp.zeros((strips, 5, GROUP, LANES), jnp.float32)

    def count(sem, blocks, rows):
        piece = images.at[pl.ds(0, blocks), pl.ds(0, rows)]
        pltpu.make_async_copy(piece, piece, sem).wait()

    def chunk_rows(chunk):
        return begins[chunk + 1] - begins[chunk] + (RADIUS if chunk == 0 else 0)

    def passed_on(beside, source, target, place):
        return [
            pltpu.make_async_remote_copy(
                src_ref=images.at[pl.ds(base + 1, strips), pl.ds(source, RADIUS)],
                dst_ref=images.at[pl.ds(base + 1, strips), pl.ds(target, RADIUS)],
                send_sem=edge_send_sem.at[place],
                recv_sem=edge_recv_sem.at[place],
                device_id={"tile": beside},
                device_id_type=MESH,
            )
            for base in (0, moving_at)
        ]

    for copy in own_copies:
        copy.wait()
    count(recv_sem.at[0], blocks, chunk_rows(0))

    @pl.when(me > 0)
    def _():
        for copy in passed_on(me - 1, RADIUS, whole - RADIUS, 0):
            copy.start()

    @pl.when(me < last)
    def _():
        for copy in passed_on(me + 1, whole - 2 * RADIUS, 0, 1):
            copy.start()

    for chunk in range(2, chunks - 1):
        send_range(chunk, 0, last, backward=True)
    send_range(chunks - 1, 0, last, True, both_images[1:], chunks - 1)
    send_range(chunks - 1, 0, last, True, both_images[:1], chunks)
    offsets_copy.wait()
    fractions_copy.wait()

    lane = lax.broadcasted_iota(jnp.int32, (GROUP, LANES), 1)

    def moved(shift, base, strip, rows):
        centre = images[base + strip + 1, rows, :]
        if shift > 0:
            right = images[base + strip + 2, rows, :]
            return pltpu.roll(jnp.where(lane < shift, right, centre), LANES - shift, 1)
        if shift < 0:
            left = images[base + strip, rows, :]
            return pltpu.roll(jnp.where(lane >= LANES + shift, left, centre), -shift, 1)
        return centre

    shifts = range(-RADIUS, RADIUS + 1)

    def image_moved(base, strip, row):
        return [moved(shift, base, strip, pl.ds(row, GROUP)) for shift in shifts]

    def moved_before(strip, row):
        rows = pl.ds(row, GROUP)
        return [
            shifted[strip, KEPT_SHIFTS.index(shift), rows, :]
            if shift
            else images[moving_at + 1 + strip, rows, :]
            for shift in shifts
        ]

    def keep(strip, row, moving_moved, kept):
        for shift, m in zip(shifts, moving_moved):
            if shift in kept:
                shifted[strip, KEPT_SHIFTS.index(shift), pl.ds(row, GROUP), :] = m

    def sums_of_three(strip, row):
        for place in range(5):
            triples[strip, place, pl.ds(row + GROUP - 2, GROUP), :] = (
                sums[strip, place, pl.ds(row + GROUP, GROUP), :]
                + sums[strip, place, pl.ds(row + GROUP - 1, GROUP), :]
                + sums[strip, place, pl.ds(row + GROUP - 2, GROUP), :]
            )

    def store_sums(strip, row, terms_of_shifts):
        totals = {}
        for terms in terms_of_shifts:
            for place, term in terms.items():
                totals[place] = totals[place] + term if place in totals else term
        for place, total in totals.items():
            sums[strip, place, pl.ds(row + GROUP, GROUP), :] = total

    def row_sums(strip, row):
        fixed_moved = image_moved(0, strip, row)
        moving_moved = image_moved(moving_at, strip, row)
        keep(strip, row, moving_moved, KEPT_SHIFTS[:-1])
        store_sums(
            strip,
            row,
            [
                {0: f, 1: m, 2: f * f, 3: m * m, 4: f * m}
                for f, m in zip(fixed_moved, moving_moved)
            ],
        )

    def row_sums_of_moving(strip, row):
        moving_moved = image_moved(moving_at, strip, row)
        keep(strip, row, moving_moved, KEPT_SHIFTS)
        store_sums(strip, row, [{1: m, 3: m * m} for m in moving_moved])

    def row_sums_with_fixed(strip, row):
        pairs = zip(image_moved(0, strip, row), moved_before(strip, row))
        store_sums(strip, row, [{0: f, 2: f * f, 4: f * m} for f, m in pairs])

    window_count = float((2 * RADIUS + 1) ** 2)

    def confidence(strip, row):
        windows = []
        for place in range(5):
            total = triples[strip, place, pl.ds(row + GROUP, GROUP), :]
            for step in (3, 6):
                total = total + triples[strip, place, pl.ds(row + GROUP + step, GROUP), :]
            windows.append(total)
        fixed_sum, moving_sum, fixed_square, moving_square, cross_sum = windows
        fixed_var = fixed_square - fixed_sum * fixed_sum * (1.0 / window_count)
        moving_var = moving_square - moving_sum * moving_sum * (1.0 / window_count)
        covariance = cross_sum - fixed_sum * moving_sum * (1.0 / window_count)
        correlation = covariance * lax.rsqrt(fixed_var * moving_var + 0.001)
        return 0.5 * (1.0 + correlation)

    def pick(values, index):
        for bit in (4, 2, 1):
            chosen = jnp.bitwise_and(index, bit) != 0
            values = [
                jnp.where(chosen, values[place + bit], values[place])
                if place + bit < len(values)
                else values[place]
                for place in range(bit + 1)
            ]
        return values

    def band_place(strip, row):
        return pl.ds(row, GROUP), pl.ds(pl.multiple_of(strip * LANES, LANES), LANES)

    def corners(strip, row):
        here = band_place(strip, row)
        column_index = offsets_buf[(1,) + here] + REACH
        row_index = offsets_buf[(0,) + here] + REACH
        lefts, rights = [], []
        for row_shift in range(-REACH, REACH + 2):
            columns = moved_before(strip, row + RADIUS + row_shift)
            left, right = pick(columns[RADIUS - REACH :], column_index)
            lefts.append(left)
            rights.append(right)
        return pick(lefts, row_index) + pick(rights, row_index)

    def blend(strip, row, top_left, bottom_left, top_right, bottom_right):
        here = band_place(strip, row)
        weight = confidence(strip, row)
        row_weight = weight * fractions_buf[(0,) + here]
        column_weight = weight * fractions_buf[(1,) + here]
        upper = (1.0 - column_weight) * top_left + column_weight * top_right
        lower = (1.0 - column_weight) * bottom_left + column_weight * bottom_right
        out_ref[here] = (1.0 - row_weight) * upper + row_weight * lower

    def group_step(group, carry):
        row = pl.multiple_of(group * GROUP, GROUP)
        for chunk in range(1, chunks - 1):
            pl.when(group == sum(CHUNKS[:chunk]))(
                functools.partial(count, recv_sem.at[chunk], blocks, chunk_rows(chunk))
            )

        def sums_step(strip, carry):
            row_sums(strip, row + GROUP)
            sums_of_three(strip, row + GROUP)
            return carry

        def warp_step(strip, carry):
            blend(strip, row, *corners(strip, row))
            return carry

        lax.fori_loop(0, strips, sums_step, 0, unroll=16)
        lax.fori_loop(0, strips, warp_step, 0, unroll=4)
        return carry

    pl.when(me < last)(functools.partial(count, edge_recv_sem.at[0], 2 * strips, RADIUS))
    pl.when(me > 0)(functools.partial(count, edge_recv_sem.at[1], 2 * strips, RADIUS))

    def edge_step(strip, carry):
        row_sums(strip, 0)
        sums_of_three(strip, 0)
        row_sums(strip, band)
        return carry

    lax.fori_loop(0, strips, edge_step, 0, unroll=2)
    lax.fori_loop(0, band // GROUP - 2, group_step, 0)

    last_rows = band - GROUP
    last_groups = (band - 2 * GROUP, band - GROUP)

    def moving_step(strip, carry):
        row_sums_of_moving(strip, last_rows)
        return carry

    def corner_step(strip, carry):
        for group, row in enumerate(last_groups):
            for place, value in enumerate(corners(strip, row)):
                corner_buf[group, place, strip] = value
        return carry

    def fixed_step(strip, carry):
        row_sums_with_fixed(strip, last_rows)
        sums_of_three(strip, last_rows)
        sums_of_three(strip, band)
        return carry

    def blend_step(strip, carry):
        for group, row in enumerate(last_groups):
            blend(strip, row, *(corner_buf[group, place, strip] for place in range(4)))
        return carry

    count(recv_sem.at[chunks - 1], blocks // 2, chunk_rows(chunks - 1))
    lax.fori_loop(0, strips, moving_step, 0, unroll=16)
    lax.fori_loop(0, strips, corner_step, 0, unroll=4)
    count(recv_sem.at[chunks], blocks // 2, chunk_rows(chunks - 1))
    lax.fori_loop(0, strips, fixed_step, 0, unroll=16)
    lax.fori_loop(0, strips, blend_step, 0, unroll=8)

    pl.when(me > 0)(functools.partial(count, edge_send_sem.at[0], 2 * strips, RADIUS))
    pl.when(me < last)(functools.partial(count, edge_send_sem.at[1], 2 * strips, RADIUS))
    for chunk in range(chunks - 1):
        count(send_sem.at[chunk], blocks, chunk_rows(chunk))
    for place in (chunks - 1, chunks):
        count(send_sem.at[place], blocks // 2, chunk_rows(chunks - 1))


def solution(mesh):
    strips = mesh.shape["tile"]

    def on_device(fixed, moving, offsets, fractions):
        band, width = offsets.shape[1:]
        padded = band + 2 * RADIUS + 2 * GROUP
        chunks = len(CHUNKS)
        return pl.pallas_call(
            functools.partial(kernel, strips),
            out_shape=pltpu.VMEM((band, width), jnp.float32),
            in_specs=[pl.BlockSpec(memory_space=pltpu.HBM)] * 4,
            out_specs=pl.BlockSpec(memory_space=pltpu.VMEM),
            scratch_shapes=[
                pltpu.VMEM((2 * (strips + 2), padded, LANES), jnp.float32),
                pltpu.VMEM((strips, len(KEPT_SHIFTS), padded, LANES), jnp.float32),
                pltpu.VMEM((strips, 5, padded, LANES), jnp.float32),
                pltpu.VMEM((strips, 5, padded, LANES), jnp.float32),
                pltpu.VMEM(offsets.shape, offsets.dtype),
                pltpu.VMEM(fractions.shape, fractions.dtype),
                pltpu.SemaphoreType.DMA((chunks + 1,)),
                pltpu.SemaphoreType.DMA((chunks + 1,)),
                pltpu.SemaphoreType.DMA((4,)),
                pltpu.SemaphoreType.REGULAR((3,)),
                pltpu.SemaphoreType.DMA((2,)),
                pltpu.SemaphoreType.DMA((2,)),
                pltpu.VMEM((2, 4, strips, GROUP, LANES), jnp.float32),
            ],
            compiler_params=pltpu.CompilerParams(
                collective_id=0, has_side_effects=True, vmem_limit_bytes=60 * 2**20
            ),
        )(fixed, moving, offsets, fractions)

    placed = (
        P("pair", "tile"),
        P("pair", "tile"),
        P(None, ("pair", "tile"), None),
        P(None, ("pair", "tile"), None),
    )
    return jax.shard_map(
        on_device, mesh=mesh, in_specs=placed, out_specs=P(("pair", "tile"), None), check_vma=False
    )
```
